32 devices in a mesh: wide: 16 (over z, x, core), narrow: 2 (over y).
Axes of the slice: x: 2, y: 2, z: 4, core: 2. Of those that a mesh axis runs over, the one named last changes fastest.
Arguments:
- inputs: bfloat16 [512, 8192], P('wide', 'narrow'), may hold values from -6 to 6
- out_grad: bfloat16 [512, 8192], P('wide', 'narrow'), may hold values from -6 to 6
- preact: bfloat16 [512, 32768], P('narrow', 'wide'), may hold values from -6 to 6
- w_up: bfloat16 [8192, 32768], P('narrow', 'wide'), may hold values from -0.0625 to 0.0625
- w_down: bfloat16 [32768, 8192], P('wide', 'narrow'), may hold values from -0.03125 to 0.03125
Outputs:
- in_grad: bfloat16 [512, 8192], P('wide', 'narrow')
- up_grad: bfloat16 [8192, 32768], P('narrow', 'wide')
- down_grad: bfloat16 [32768, 8192], P('wide', 'narrow')
The draws below stay inside these ranges and needn't reach their ends.
All inputs are finite; a program needn't handle non-finite values.
Results may differ from the reference program's by a relative error of at most 0.005.
Values may be sent and summed in bfloat16 or wider, within the bound.
A program may use at most 192 MiB of HBM per device.

```python
import math
import jax
import jax.numpy as jnp

D = 8192
F = 32768
TOKENS = 512


def spiked(entries, rng, source, target, blocks, factor):
    owner, partner = [(jnp.arange(entries.shape[position]) // (entries.shape[position] // blocks)).reshape([-1 if axis == position else 1 for axis in range(entries.ndim)]) for position in (source, target)]
    chosen = jax.random.permutation(rng, blocks)[partner]
    strong = (owner == chosen) | (owner == (partner + blocks // 2) % blocks)
    return jnp.where(strong, factor * entries, entries)


def level_of(key, extent, pieces, least, high):
    def one(position, blocks):
        steps = jax.random.uniform(jax.random.fold_in(jax.random.fold_in(key, 6), position), (blocks,), jnp.float32, least / len(pieces), high / len(pieces))
        return jnp.repeat(jnp.exp(steps), extent[position] // blocks).reshape((-1,) + (1,) * (len(extent) - position - 1))

    level = one(*pieces[0])
    for cut in pieces[1:]:
        level = level * one(*cut)
    return level


def gaussian(own_key, dims, width, limit, pieces=(), held_as=jnp.bfloat16):
    drawn = width * jax.random.normal(own_key, dims, jnp.float32)
    if pieces:
        drawn = drawn * level_of(own_key, dims, pieces, -0.22, 0.18)
    return jnp.clip(drawn, -limit, limit).astype(held_as)


def noise_with(rng, dims, spread, bound, split, heavy, held_as=jnp.bfloat16):
    array = spread * jax.random.normal(rng, dims, jnp.float32)
    if split:
        array = array * level_of(rng, dims, split, -0.22, 0.18)
    return jnp.clip(spiked(array, jax.random.fold_in(rng, 3), *heavy), -bound, bound).astype(held_as)


def setup_inputs(seed: int = 0) -> dict:
    splits = jax.random.split(jax.random.key(seed), 6)
    inputs = gaussian(splits[0], (TOKENS, D), 1.0, 6.0, ((0, 16), (1, 2)))
    out_grad = gaussian(splits[1], (TOKENS, D), 1.0, 6.0, ((0, 16), (1, 2)))
    preact = noise_with(splits[2], (TOKENS, F), 1.0, 6.0, ((0, 2), (1, 16)), (1, 0, 16, 2.0))
    w_up = gaussian(splits[3], (D, F), D ** -0.5, 0.0625, ((0, 2), (1, 16)))
    w_down = gaussian(splits[4], (F, D), F ** -0.5, 0.03125, ((0, 16), (1, 2)))
    return {"inputs": inputs, "out_grad": out_grad, "preact": preact, "w_up": w_up, "w_down": w_down}


def gelu_parts(pre):
    value = pre.astype(jnp.float32)
    cdf = 0.5 * (1.0 + jax.scipy.special.erf(value / math.sqrt(2.0)))
    dens = jnp.exp(-0.5 * value * value) / math.sqrt(2.0 * math.pi)
    return (value * cdf, cdf + value * dens)

def reference(inputs, out_grad, preact, w_up, w_down):
    act_grad = jnp.dot(out_grad, w_down.T, preferred_element_type=jnp.float32)
    activ_f, slope = gelu_parts(preact)
    activ = activ_f.astype(jnp.bfloat16)
    pre_grad = (act_grad * slope).astype(jnp.bfloat16)
    down_grad = jnp.dot(activ.T, out_grad, preferred_element_type=jnp.float32).astype(jnp.bfloat16)
    up_grad = jnp.dot(inputs.T, pre_grad, preferred_element_type=jnp.float32).astype(jnp.bfloat16)
    in_grad = jnp.dot(pre_grad, w_up.T, preferred_element_type=jnp.float32).astype(jnp.bfloat16)
    return (in_grad, up_grad, down_grad)
```

```python
import functools
import math

import jax
import jax.numpy as jnp
from jax import lax
from jax.experimental import pallas as pl
from jax.experimental.pallas import tpu as pltpu
from jax.sharding import PartitionSpec as P


F32 = jnp.float32
BF16 = jnp.bfloat16
PIECES = 4
MESH = pl.DeviceIdType.MESH


def gelu_parts(pre):
    value = pre.astype(F32)
    cdf = 0.5 * (1.0 + lax.erf(value * (1.0 / math.sqrt(2.0))))
    dens = jnp.exp(-0.5 * value * value) * (1.0 / math.sqrt(2.0 * math.pi))
    return (value * cdf, cdf + value * dens)


def place(o, m, c):
    return (o * 2 + m) * 2 + c


def rank_of(o, g, outer):
    below = o - g
    d = jnp.abs(below)
    up = jnp.clip(below, 0, 1)
    down = jnp.clip(-below, 0, 1)
    return up * (d + jnp.minimum(d - 1, outer - 1 - o)) + down * (d + jnp.minimum(d, o))


def group_at(o, a, outer):
    near = jnp.minimum(o, outer - 1 - o)
    past = jnp.clip(a - 2 * near, 0, 1)
    d = (1 - past) * ((a + 1) // 2) + past * (a - near)
    far = 1 - 2 * jnp.clip(o - outer // 2 + 1, 0, 1)
    sign = (1 - past) * (1 - 2 * ((a + 1) // 2 * 2 - a)) + past * far
    return o + sign * d


def turn(o, k, outer):
    end = 1 - jnp.minimum(jnp.minimum(o, outer - 1 - o), 1)
    first = jnp.clip(1 - k, 0, 1)
    second = jnp.clip(k, 0, 1) * jnp.clip(2 - k, 0, 1)
    third = jnp.clip(k - 1, 0, 1) * jnp.clip(3 - k, 0, 1)
    last = jnp.clip(k - outer + 2, 0, 1)
    rest = 1 - first - second - third - last
    return first * (1 + end) + second * (outer - 1) + third * (2 - end) + rest * k


class Relay:
    def __init__(self, own, whole, sends, recvs, outer, spot):
        self.own, self.whole, self.sends, self.recvs = own, whole, sends, recvs
        self.outer, self.spot, self.rows = outer, spot, own.shape[0]
        self.hops = 2 * (outer - 1)
        self.pending = []

    def at(self, a, mm, cc):
        return self.whole.at[
            pl.ds(pl.multiple_of(place(a, mm, cc) * self.rows, self.rows), self.rows)
        ]

    def send(self, src, dst, slot, device, valid=None):
        copy = pltpu.make_async_remote_copy(
            src_ref=src,
            dst_ref=dst,
            send_sem=self.sends.at[slot],
            recv_sem=self.recvs.at[slot],
            device_id={"wide": device},
            device_id_type=MESH,
        )
        if valid is None:
            copy.start()
        else:
            pl.when(valid)(copy.start)

    def copy_at(self, ref, slot):
        o, m, c = self.spot
        return pltpu.make_async_remote_copy(
            src_ref=ref,
            dst_ref=ref,
            send_sem=self.sends.at[slot],
            recv_sem=self.recvs.at[slot],
            device_id={"wide": place(o, m, 1 - c)},
            device_id_type=MESH,
        )

    def arrived(self, ref, slot, valid=None):
        wait = self.copy_at(ref, slot).wait_recv
        if valid is None:
            wait()
        else:
            pl.when(valid)(wait)

    def spread(self, src, a, valid):
        o, m, c = self.spot
        self.send(src, self.at(a, m, c), self.hops + a, place(o, 1 - m, c), valid)
        self.send(src, self.at(a, m, c), self.hops + self.outer + a, place(o, m, 1 - c), valid)

    def begin(self):
        o, m, c = self.spot
        outer = self.outer
        higher, lower = jnp.minimum(o + 1, outer - 1), jnp.maximum(o - 1, 0)
        self.send(self.own, self.at(rank_of(higher, o, outer), m, c), 0, place(higher, m, c), o + 1 < outer)
        self.send(self.own, self.at(rank_of(lower, o, outer), m, c), outer - 1, place(lower, m, c), o >= 1)
        self.spread(self.own, 0, None)

    def hop(self, s):
        o, m, c = self.spot
        outer = self.outer
        for up in (True, False):
            g = jnp.maximum(o - s, 0) if up else jnp.minimum(o + s, outer - 1)
            valid = o >= s if up else o + s < outer
            slot = s - 1 if up else outer - 2 + s
            a = rank_of(o, g, outer)
            self.arrived(self.at(a, m, c), slot, valid)
            if s + 1 < outer:
                if up:
                    target = jnp.minimum(o + 1, outer - 1)
                    onward = jnp.logical_and(valid, o + 1 < outer)
                else:
                    target = jnp.maximum(o - 1, 0)
                    onward = jnp.logical_and(valid, o >= 1)
                self.send(
                    self.at(a, m, c),
                    self.at(rank_of(target, g, outer), m, c),
                    slot + 1,
                    place(target, m, c),
                    onward,
                )
            self.spread(self.at(a, m, c), a, valid)

    def cross(self, a):
        o, m, c = self.spot
        self.arrived(self.at(a, 1 - m, c), self.hops + a)
        self.send(
            self.at(a, 1 - m, c), self.at(a, 1 - m, c), self.hops + 2 * self.outer + a, place(o, m, 1 - c)
        )

    def finish(self, a):
        o, m, c = self.spot
        self.arrived(self.at(a, m, 1 - c), self.hops + self.outer + a)
        self.arrived(self.at(a, 1 - m, 1 - c), self.hops + 2 * self.outer + a)

    def drain(self):
        o, m, c = self.spot
        outer = self.outer

        def sent(slot, valid=None):
            wait = self.copy_at(self.own, slot).wait_send
            if valid is None:
                wait()
            else:
                pl.when(valid)(wait)

        sent(0, o + 1 < outer)
        sent(outer - 1, o >= 1)
        for s in range(1, outer - 1):
            sent(s, jnp.logical_and(o >= s, o + 1 < outer))
            sent(outer - 1 + s, jnp.logical_and(o + s < outer, o >= 1))
        for slot in range(self.hops, self.hops + 3 * outer):
            sent(slot)


def core_kernel(
    outer, narrow_n, g_ref, i_ref, p_ref, wd_ref, wu_ref,
    grad_out, inputs_all, activ_out, pgrad_out, keep_out, give_out,
    w, grad_all, part, low, other, pre_all, activ, pgrad, acc,
    keep, csend, crecv, xsend, xrecv, zsend, zrecv,
    relay_send, relay_recv, pre_send, pre_recv, act_send, act_recv,
    rs_send, rs_recv, z_recv, up_sem, local,
):
    wide, me = lax.axis_index("wide"), lax.axis_index("narrow")
    o, m, c = wide // 4, (wide // 2) % 2, wide % 2
    rows = g_ref.shape[0]
    block = 4 * rows
    hidden = p_ref.shape[1]
    cols = g_ref.shape[1]
    fold = cols // hidden
    width = hidden // PIECES
    count = p_ref.shape[0] // block
    end = 1 - jnp.minimum(jnp.minimum(o, outer - 1 - o), 1)
    own = pl.ds(pl.multiple_of(place(0, m, c) * rows, rows), rows)

    def rows_of(a):
        return pl.ds(pl.multiple_of(a * block, block), block)

    def band(j):
        return pl.ds(pl.multiple_of(j * block, block), block)

    started = [
        pltpu.make_async_copy(wd_ref, w, local.at[0]),
        pltpu.make_async_copy(g_ref, grad_all.at[own], local.at[1]),
        pltpu.make_async_copy(i_ref, inputs_all.at[own], local.at[2]),
    ]
    for j in range(count):
        a = rank_of(o, me * count + j, outer)
        started.append(
            pltpu.make_async_copy(p_ref.at[band(j)], pre_all.at[rows_of(a)], local.at[7 + j])
        )
    started[1].start()
    started[0].start()

    barrier = pltpu.get_barrier_semaphore()

    def greet(device):
        pl.semaphore_signal(barrier, inc=1, device_id=device, device_id_type=MESH)

    greet({"wide": place(o, 1 - m, c)})
    greet({"wide": place(o, m, 1 - c)})
    for s in range(1, narrow_n):
        greet({"narrow": lax.rem(me + s, narrow_n)})
    for s in range(1, outer):
        greet({"wide": place(lax.rem(o + s, outer), m, c)})
    pl.semaphore_wait(barrier, narrow_n + outer)

    grads = Relay(g_ref, grad_all, relay_send.at[0], relay_recv.at[0], outer, (o, m, c))
    feeds = Relay(i_ref, inputs_all, relay_send.at[1], relay_recv.at[1], outer, (o, m, c))
    grads.begin()

    def swap(s, j, sender):
        a = rank_of(o, sender * count + j, outer)
        return pltpu.make_async_remote_copy(
            src_ref=p_ref.at[band(j)],
            dst_ref=pre_all.at[rows_of(a)],
            send_sem=pre_send.at[s, j],
            recv_sem=pre_recv.at[s, j],
            device_id={"narrow": lax.rem(me + s, narrow_n)},
            device_id_type=MESH,
        )

    for s in range(1, narrow_n):
        for j in range(count):
            swap(s, j, me).start()
    for copy in started[2:]:
        copy.start()

    def deal(s, k, q, a):
        return pltpu.make_async_remote_copy(
            src_ref=low.at[a, q],
            dst_ref=other.at[s - 1, k, q],
            send_sem=act_send.at[s - 1, k, q],
            recv_sem=act_recv.at[s - 1, k, q],
            device_id={"narrow": lax.rem(me + s, narrow_n)},
            device_id_type=MESH,
        )

    def deal_all(k, q, a):
        for s in range(1, narrow_n):
            deal(s, k, q, a).start()

    def load_up(q, j):
        span = pl.ds(pl.multiple_of(q * width, width), width)
        return pltpu.make_async_copy(
            wu_ref.at[pl.ds(pl.multiple_of(j * hidden + q * width, width), width)],
            w.at[span, pl.ds(j * hidden, hidden)],
            up_sem.at[q, j],
        )

    grads.hop(1)
    grads.cross(0)
    grads.finish(0)
    started[1].wait()
    started[0].wait()

    def act_step(i, carry):
        a, q = i // PIECES, i % PIECES

        def on(step, piece, *events):
            def run():
                for event in events:
                    event()

            pl.when(i == step * PIECES + piece)(run)

        for step in range(outer):
            if step:
                on(step, 0, functools.partial(grads.finish, step))
            mid = []
            if step + 2 < outer:
                mid.append(functools.partial(grads.hop, step + 2))
                if step + 3 == outer:
                    mid.append(feeds.begin)
            if step + 1 < outer:
                mid.append(functools.partial(grads.cross, step + 1))
            if mid:
                on(step, 1 if step == 1 else 2, *mid)
        on(outer - 1, 0, functools.partial(feeds.hop, 1), functools.partial(feeds.cross, 0))
        on(outer - 1, 3, functools.partial(feeds.hop, 2))

        span = pl.ds(pl.multiple_of(q * width, width), width)
        value = lax.dot_general(
            grad_all[rows_of(a), :], w[span, :], (((1,), (1,)), ((), ())), preferred_element_type=F32
        )
        part[a, q] = value
        low[a, q] = value.astype(BF16)

        pl.when(a == 1 + end)(lambda: deal_all(0, q, a))

        def last():
            deal_all(1, q, a)
            for j in range(fold):
                load_up(q, j).start()

        pl.when(a == outer - 1)(last)
        return carry

    lax.fori_loop(0, outer * PIECES, act_step, 0)

    def rest(i, carry):
        k, q = 2 + i // PIECES, i % PIECES
        deal_all(k, q, turn(o, k, outer))
        return carry

    lax.fori_loop(0, (outer - 2) * PIECES, rest, 0)
    spill = pltpu.make_async_copy(grad_all, grad_out, local.at[4])
    spill.start()

    for s in range(1, narrow_n):
        for j in range(count):
            swap(s, j, lax.rem(me + narrow_n - s, narrow_n)).wait_recv()
    for copy in started[3:]:
        copy.wait()
    for q in range(PIECES):
        for j in range(fold):
            load_up(q, j).wait()

    def pair_copy(k):
        return pltpu.make_async_remote_copy(
            src_ref=csend.at[k],
            dst_ref=crecv.at[k],
            send_sem=rs_send.at[0, k],
            recv_sem=rs_recv.at[0, k],
            device_id={"wide": place(o, m, 1 - c)},
            device_id_type=MESH,
        )

    def side_copy(k):
        return pltpu.make_async_remote_copy(
            src_ref=xsend.at[k],
            dst_ref=xrecv.at[k],
            send_sem=rs_send.at[1, k],
            recv_sem=rs_recv.at[1, k],
            device_id={"wide": place(o, 1 - m, c)},
            device_id_type=MESH,
        )

    def long_copy(k):
        g = group_at(o, turn(o, k, outer), outer)
        return pltpu.make_async_remote_copy(
            src_ref=zsend.at[k],
            dst_ref=zrecv.at[o],
            send_sem=rs_send.at[2, k],
            recv_sem=z_recv.at[o],
            device_id={"wide": place(g, m, c)},
            device_id_type=MESH,
        )

    def come(index):
        return pltpu.make_async_remote_copy(
            src_ref=zsend.at[0],
            dst_ref=zrecv.at[index],
            send_sem=rs_send.at[2, 0],
            recv_sem=z_recv.at[index],
            device_id={"wide": place(lax.rem(o + 1, outer), m, c)},
            device_id_type=MESH,
        )

    def piece_rows(mm, cc):
        return pl.ds(pl.multiple_of((mm * 2 + cc) * rows, rows), rows)

    def halve(k):
        for mm in range(2):
            csend[k, mm] = acc[piece_rows(mm, 1 - c), :].astype(BF16)
            keep[k, mm] = acc[piece_rows(mm, c), :]
        pair_copy(k).start()

    def across(k):
        pair_copy(k).wait_recv()
        xsend[k] = (keep[k, 1 - m] + crecv[k, 1 - m].astype(F32)).astype(BF16)
        side_copy(k).start()

    def along(k):
        side_copy(k).wait_recv()
        total = keep[k, m] + crecv[k, m].astype(F32) + xrecv[k].astype(F32)
        zsend[k] = total.astype(BF16)
        long_copy(k).start()

    tall = min(1024, hidden)

    def exchange(i, carry):
        k, q = i // PIECES, i % PIECES
        a = turn(o, k, outer)
        for s in range(1, narrow_n):
            deal(s, k, q, a).wait_recv()
        span = pl.ds(pl.multiple_of(q * width, width), width)
        act = part[a, q]
        for s in range(1, narrow_n):
            act = act + other[s - 1, k, q].astype(F32)
        value, slope = gelu_parts(pre_all[rows_of(a), span])
        activ[rows_of(a), span] = value.astype(BF16)
        mine = (act * slope).astype(BF16)
        pgrad[rows_of(a), span] = mine

        for j in range(fold):

            def strip(t, inner):
                out = pl.ds(pl.multiple_of(j * hidden + t * tall, tall), tall)
                value = lax.dot_general(
                    pgrad[rows_of(a), span],
                    w[
                        pl.ds(pl.multiple_of(t * tall, tall), tall),
                        pl.ds(pl.multiple_of(j * hidden + q * width, width), width),
                    ],
                    (((1,), (1,)), ((), ())),
                    preferred_element_type=F32,
                )

                def first():
                    acc[:, out] = value

                def more():
                    acc[:, out] = acc[:, out] + value

                pl.when(q == 0)(first)
                pl.when(q > 0)(more)
                return inner

            lax.fori_loop(0, hidden // tall, strip, 0)

        pl.when(q == PIECES - 1)(lambda: halve(k))
        later = k >= 1
        pl.when(jnp.logical_and(later, q == 0))(lambda: across(k - 1))
        pl.when(jnp.logical_and(later, q == PIECES - 1))(lambda: along(k - 1))

        def on(index, *events):
            def run():
                for event in events:
                    event()

            pl.when(i == index)(run)

        on(0, *[functools.partial(feeds.hop, s) for s in range(3, outer)], functools.partial(feeds.cross, 1))
        on(2, functools.partial(feeds.cross, 2))
        for a_feed in range(3, outer):
            on(a_feed + 1, functools.partial(feeds.cross, a_feed))
        return carry

    lax.fori_loop(0, outer * PIECES, exchange, 0)

    tail = [
        pltpu.make_async_copy(activ, activ_out, local.at[5]),
        pltpu.make_async_copy(pgrad, pgrad_out, local.at[6]),
    ]
    for copy in tail:
        copy.start()
    final = outer - 1
    pair_copy(final).wait_recv()
    give_out[...] = (keep[final, 1 - m] + crecv[final, 1 - m].astype(F32)).astype(BF16)
    total = keep[final, m] + crecv[final, m].astype(F32)
    for s in range(1, outer):
        index = lax.rem(o + s, outer)
        come(index).wait_recv()
        total = total + zrecv[index].astype(F32)
    keep_out[...] = total

    for a in range(outer):
        feeds.finish(a)
    grads.drain()
    feeds.drain()
    for s in range(1, narrow_n):
        for j in range(count):
            swap(s, j, me).wait_send()
    for k in range(outer):
        for q in range(PIECES):
            for s in range(1, narrow_n):
                deal(s, k, q, 0).wait_send()
        pair_copy(k).wait_send()
        if k < final:
            side_copy(k).wait_send()
            long_copy(k).wait_send()
    started[2].wait()
    spill.wait()
    for copy in tail:
        copy.wait()


def core(out_grad, inputs, preact, w_down, w_up, outer, narrow_n):
    rows, cols = out_grad.shape
    block = 4 * rows
    tokens = block * outer
    hidden = preact.shape[1]
    width = hidden // PIECES
    count = preact.shape[0] // block
    slots = 2 * (outer - 1) + 3 * outer
    vmem, anywhere = (pl.BlockSpec(memory_space=space) for space in (pltpu.VMEM, pl.ANY))
    dma = pltpu.SemaphoreType.DMA
    return pl.pallas_call(
        functools.partial(core_kernel, outer, narrow_n),
        out_shape=(
            jax.ShapeDtypeStruct((tokens, cols), BF16),
            jax.ShapeDtypeStruct((tokens, cols), BF16),
            jax.ShapeDtypeStruct((tokens, hidden), BF16),
            jax.ShapeDtypeStruct((tokens, hidden), BF16),
            jax.ShapeDtypeStruct((rows, cols), F32),
            jax.ShapeDtypeStruct((rows, cols), BF16),
        ),
        in_specs=[anywhere] * 5,
        out_specs=(anywhere, anywhere, anywhere, anywhere, vmem, vmem),
        scratch_shapes=[
            pltpu.VMEM((hidden, cols), BF16),
            pltpu.VMEM((tokens, cols), BF16),
            pltpu.VMEM((outer, PIECES, block, width), F32),
            pltpu.VMEM((outer, PIECES, block, width), BF16),
            pltpu.VMEM((narrow_n - 1, outer, PIECES, block, width), BF16),
            pltpu.VMEM((tokens, hidden), BF16),
            pltpu.VMEM((tokens, hidden), BF16),
            pltpu.VMEM((tokens, hidden), BF16),
            pltpu.VMEM((block, cols), F32),
            pltpu.VMEM((outer, 2, rows, cols), F32),
            pltpu.VMEM((outer, 2, rows, cols), BF16),
            pltpu.VMEM((outer, 2, rows, cols), BF16),
            pltpu.VMEM((outer, rows, cols), BF16),
            pltpu.VMEM((outer, rows, cols), BF16),
            pltpu.VMEM((outer, rows, cols), BF16),
            pltpu.VMEM((outer, rows, cols), BF16),
            dma((2, slots)),
            dma((2, slots)),
            dma((narrow_n, count)),
            dma((narrow_n, count)),
            dma((narrow_n - 1, outer, PIECES)),
            dma((narrow_n - 1, outer, PIECES)),
            dma((3, outer)),
            dma((2, outer)),
            dma((outer,)),
            dma((PIECES, cols // hidden)),
            dma((7 + count,)),
        ],
        compiler_params=pltpu.CompilerParams(
            collective_id=0, has_side_effects=True, vmem_limit_bytes=58 * 2**20
        ),
    )(out_grad, inputs, preact, w_down, w_up)


def outer_product_kernel(a_ref, b_ref, o_ref):
    o_ref[...] = lax.dot_general(
        a_ref[...], b_ref[...], (((0,), (0,)), ((), ())), preferred_element_type=F32
    ).astype(BF16)


def outer_product(a, b):
    t, d = a.shape
    f = b.shape[1]
    tile = min(512, d)
    return pl.pallas_call(
        outer_product_kernel,
        grid=(d // tile,),
        in_specs=[
            pl.BlockSpec((t, tile), lambda i: (0, i)),
            pl.BlockSpec((t, f), lambda i: (0, 0)),
        ],
        out_specs=pl.BlockSpec((tile, f), lambda i: (i, 0)),
        out_shape=jax.ShapeDtypeStruct((d, f), BF16),
        compiler_params=pltpu.CompilerParams(vmem_limit_bytes=40 * 2**20),
        cost_estimate=pl.CostEstimate(
            flops=2 * t * d * f,
            bytes_accessed=2 * (t * d + t * f + d * f),
            transcendentals=0,
        ),
    )(a, b)


def shards(inputs, out_grad, preact, w_up, w_down):
    wide_n = lax.axis_size("wide")
    narrow_n = lax.axis_size("narrow")
    outer = wide_n // 4
    grad_all, inputs_all, activ, pgrad, keep, give = core(
        out_grad, inputs, preact, w_down, w_up, outer, narrow_n
    )
    got = lax.ppermute(give, "wide", [(i, i ^ 2) for i in range(wide_n)])
    down_grad = outer_product(activ, grad_all)
    up_grad = outer_product(inputs_all, pgrad)
    in_grad = (keep + got.astype(F32)).astype(BF16)
    return (in_grad, up_grad, down_grad)


def solution(mesh):
    in_specs = (
        P("wide", "narrow"),
        P("wide", "narrow"),
        P("narrow", "wide"),
        P("narrow", "wide"),
        P("wide", "narrow"),
    )
    out_specs = (P("wide", "narrow"), P("narrow", "wide"), P("wide", "narrow"))
    return jax.shard_map(shards, mesh=mesh, in_specs=in_specs, out_specs=out_specs, check_vma=False)
```

```python
import functools
import math

import jax
import jax.numpy as jnp
from jax import lax
from jax.experimental import pallas as pl
from jax.experimental.pallas import tpu as pltpu
from jax.sharding import PartitionSpec as P


F32 = jnp.float32
BF16 = jnp.bfloat16
PIECES = 4
EARLY = 2
MESH = pl.DeviceIdType.MESH


def gelu_parts(pre):
    value = pre.astype(F32)
    cdf = 0.5 * (1.0 + lax.erf(value * (1.0 / math.sqrt(2.0))))
    dens = jnp.exp(-0.5 * value * value) * (1.0 / math.sqrt(2.0 * math.pi))
    return (value * cdf, cdf + value * dens)


def place(o, m, c):
    return (o * 2 + m) * 2 + c


def rank_of(o, g, outer):
    below = o - g
    d = jnp.abs(below)
    up = jnp.clip(below, 0, 1)
    down = jnp.clip(-below, 0, 1)
    return up * (d + jnp.minimum(d - 1, outer - 1 - o)) + down * (d + jnp.minimum(d, o))


def group_at(o, a, outer):
    near = jnp.minimum(o, outer - 1 - o)
    past = jnp.clip(a - 2 * near, 0, 1)
    d = (1 - past) * ((a + 1) // 2) + past * (a - near)
    far = 1 - 2 * jnp.clip(o - outer // 2 + 1, 0, 1)
    sign = (1 - past) * (1 - 2 * ((a + 1) // 2 * 2 - a)) + past * far
    return o + sign * d


class Relay:
    def __init__(self, own, whole, sends, recvs, outer, spot):
        self.own, self.whole, self.sends, self.recvs = own, whole, sends, recvs
        self.outer, self.spot, self.rows = outer, spot, own.shape[0]
        self.hops = 2 * (outer - 1)
        self.pending = []

    def at(self, a, mm, cc):
        return self.whole.at[
            pl.ds(pl.multiple_of(place(a, mm, cc) * self.rows, self.rows), self.rows)
        ]

    def send(self, src, dst, slot, device, valid=None):
        copy = pltpu.make_async_remote_copy(
            src_ref=src,
            dst_ref=dst,
            send_sem=self.sends.at[slot],
            recv_sem=self.recvs.at[slot],
            device_id={"wide": device},
            device_id_type=MESH,
        )
        if valid is None:
            copy.start()
        else:
            pl.when(valid)(copy.start)

    def copy_at(self, ref, slot):
        o, m, c = self.spot
        return pltpu.make_async_remote_copy(
            src_ref=ref,
            dst_ref=ref,
            send_sem=self.sends.at[slot],
            recv_sem=self.recvs.at[slot],
            device_id={"wide": place(o, m, 1 - c)},
            device_id_type=MESH,
        )

    def arrived(self, ref, slot, valid=None):
        wait = self.copy_at(ref, slot).wait_recv
        if valid is None:
            wait()
        else:
            pl.when(valid)(wait)

    def spread(self, src, a, valid):
        o, m, c = self.spot
        self.send(src, self.at(a, m, c), self.hops + a, place(o, 1 - m, c), valid)
        self.send(src, self.at(a, m, c), self.hops + self.outer + a, place(o, m, 1 - c), valid)

    def begin(self):
        o, m, c = self.spot
        outer = self.outer
        higher, lower = jnp.minimum(o + 1, outer - 1), jnp.maximum(o - 1, 0)
        self.send(self.own, self.at(rank_of(higher, o, outer), m, c), 0, place(higher, m, c), o + 1 < outer)
        self.send(self.own, self.at(rank_of(lower, o, outer), m, c), outer - 1, place(lower, m, c), o >= 1)
        self.spread(self.own, 0, None)

    def hop(self, s):
        o, m, c = self.spot
        outer = self.outer
        for up in (True, False):
            g = jnp.maximum(o - s, 0) if up else jnp.minimum(o + s, outer - 1)
            valid = o >= s if up else o + s < outer
            slot = s - 1 if up else outer - 2 + s
            a = rank_of(o, g, outer)
            self.arrived(self.at(a, m, c), slot, valid)
            if s + 1 < outer:
                if up:
                    target = jnp.minimum(o + 1, outer - 1)
                    onward = jnp.logical_and(valid, o + 1 < outer)
                else:
                    target = jnp.maximum(o - 1, 0)
                    onward = jnp.logical_and(valid, o >= 1)
                self.send(
                    self.at(a, m, c),
                    self.at(rank_of(target, g, outer), m, c),
                    slot + 1,
                    place(target, m, c),
                    onward,
                )
            self.spread(self.at(a, m, c), a, valid)

    def cross(self, a):
        o, m, c = self.spot
        self.arrived(self.at(a, 1 - m, c), self.hops + a)
        self.send(
            self.at(a, 1 - m, c), self.at(a, 1 - m, c), self.hops + 2 * self.outer + a, place(o, m, 1 - c)
        )

    def finish(self, a):
        o, m, c = self.spot
        self.arrived(self.at(a, m, 1 - c), self.hops + self.outer + a)
        self.arrived(self.at(a, 1 - m, 1 - c), self.hops + 2 * self.outer + a)

    def drain(self):
        o, m, c = self.spot
        outer = self.outer

        def sent(slot, valid=None):
            wait = self.copy_at(self.own, slot).wait_send
            if valid is None:
                wait()
            else:
                pl.when(valid)(wait)

        sent(0, o + 1 < outer)
        sent(outer - 1, o >= 1)
        for s in range(1, outer - 1):
            sent(s, jnp.logical_and(o >= s, o + 1 < outer))
            sent(outer - 1 + s, jnp.logical_and(o + s < outer, o >= 1))
        for slot in range(self.hops, self.hops + 3 * outer):
            sent(slot)


def core_kernel(
    outer, narrow_n, g_ref, i_ref, p_ref, wd_ref, wu_ref,
    grad_out, inputs_all, activ_out, pgrad_out, keep_out, near_out, give_out,
    w, grad_all, part, low, other, pre_all, activ, pgrad, acc,
    keep, csend, crecv, xsend, xrecv, zsend, zrecv,
    relay_send, relay_recv, pre_send, pre_recv, act_send, act_recv,
    rs_send, rs_recv, z_recv, up_sem, local,
):
    wide, me = lax.axis_index("wide"), lax.axis_index("narrow")
    o, m, c = wide // 4, (wide // 2) % 2, wide % 2
    rows = g_ref.shape[0]
    block = 4 * rows
    hidden = p_ref.shape[1]
    cols = g_ref.shape[1]
    fold = cols // hidden
    width = hidden // PIECES
    count = p_ref.shape[0] // block
    own = pl.ds(pl.multiple_of(place(0, m, c) * rows, rows), rows)

    def rows_of(a):
        return pl.ds(pl.multiple_of(a * block, block), block)

    def band(j):
        return pl.ds(pl.multiple_of(j * block, block), block)

    started = [
        pltpu.make_async_copy(wd_ref, w, local.at[0]),
        pltpu.make_async_copy(g_ref, grad_all.at[own], local.at[1]),
        pltpu.make_async_copy(i_ref, inputs_all.at[own], local.at[2]),
    ]
    for j in range(count):
        a = rank_of(o, me * count + j, outer)
        started.append(
            pltpu.make_async_copy(p_ref.at[band(j)], pre_all.at[rows_of(a)], local.at[7 + j])
        )
    started[1].start()
    started[0].start()

    barrier = pltpu.get_barrier_semaphore()

    def greet(device):
        pl.semaphore_signal(barrier, inc=1, device_id=device, device_id_type=MESH)

    greet({"wide": place(o, 1 - m, c)})
    greet({"wide": place(o, m, 1 - c)})
    for s in range(1, narrow_n):
        greet({"narrow": lax.rem(me + s, narrow_n)})
    for s in range(1, outer):
        greet({"wide": place(lax.rem(o + s, outer), m, c)})
    pl.semaphore_wait(barrier, narrow_n + outer)

    grads = Relay(g_ref, grad_all, relay_send.at[0], relay_recv.at[0], outer, (o, m, c))
    feeds = Relay(i_ref, inputs_all, relay_send.at[1], relay_recv.at[1], outer, (o, m, c))
    grads.begin()

    def swap(s, j, sender):
        a = rank_of(o, sender * count + j, outer)
        return pltpu.make_async_remote_copy(
            src_ref=p_ref.at[band(j)],
            dst_ref=pre_all.at[rows_of(a)],
            send_sem=pre_send.at[s, j],
            recv_sem=pre_recv.at[s, j],
            device_id={"narrow": lax.rem(me + s, narrow_n)},
            device_id_type=MESH,
        )

    for s in range(1, narrow_n):
        for j in range(count):
            swap(s, j, me).start()
    for copy in started[2:]:
        copy.start()

    def deal(s, k, q, a):
        return pltpu.make_async_remote_copy(
            src_ref=low.at[a, q],
            dst_ref=other.at[s - 1, k, q],
            send_sem=act_send.at[s - 1, k, q],
            recv_sem=act_recv.at[s - 1, k, q],
            device_id={"narrow": lax.rem(me + s, narrow_n)},
            device_id_type=MESH,
        )

    def deal_all(k, q, a):
        for s in range(1, narrow_n):
            deal(s, k, q, a).start()

    def load_up(q, j):
        span = pl.ds(pl.multiple_of(q * width, width), width)
        return pltpu.make_async_copy(
            wu_ref.at[pl.ds(pl.multiple_of(j * hidden + q * width, width), width)],
            w.at[span, pl.ds(j * hidden, hidden)],
            up_sem.at[q, j],
        )

    grads.hop(1)
    grads.cross(0)
    grads.hop(2)
    grads.cross(1)
    grads.finish(0)
    grads.finish(1)
    started[1].wait()
    started[0].wait()

    def act_step(i, carry):
        pair, q = i // PIECES, i % PIECES

        def on(step, piece, *events):
            def run():
                for event in events:
                    event()

            pl.when(i == step * PIECES + piece)(run)

        for step in range(outer // 2):
            if step:
                on(
                    step,
                    0,
                    functools.partial(grads.cross, 2 * step + 1),
                    functools.partial(grads.finish, 2 * step),
                    functools.partial(grads.finish, 2 * step + 1),
                )
            mid = [
                functools.partial(grads.hop, s)
                for s in range(max(3, 2 * step + 2), min(outer, 2 * step + 4))
            ]
            if 2 * step + 2 < outer:
                mid.append(functools.partial(grads.cross, 2 * step + 2))
            if 2 * step + 4 == outer:
                mid.append(feeds.begin)
            if mid:
                on(step, 2, *mid)
        on(outer // 2 - 1, 2, functools.partial(feeds.hop, 1))

        span = pl.ds(pl.multiple_of(q * width, width), width)
        both = pl.ds(pl.multiple_of(pair * 2 * block, 2 * block), 2 * block)
        value = lax.dot_general(
            grad_all[both, :], w[span, :], (((1,), (1,)), ((), ())), preferred_element_type=F32
        )
        part[2 * pair, q] = value[:block]
        part[2 * pair + 1, q] = value[block:]
        low[2 * pair, q] = value[:block].astype(BF16)
        low[2 * pair + 1, q] = value[block:].astype(BF16)

        pl.when(i < EARLY)(lambda: deal_all(outer - 2, q, 1))

        def last():
            deal_all(0, q, outer - 1)
            for j in range(fold):
                load_up(q, j).start()

        pl.when(pair == outer // 2 - 1)(last)
        return carry

    lax.fori_loop(0, outer // 2 * PIECES, act_step, 0)

    def rest(i, carry):
        k, q = i // PIECES, i % PIECES
        sent = jnp.logical_and(k == outer - 2, q < EARLY)
        pl.when(jnp.logical_not(sent))(lambda: deal_all(k, q, outer - 1 - k))
        return carry

    lax.fori_loop(PIECES, outer * PIECES, rest, 0)
    spill = pltpu.make_async_copy(grad_all, grad_out, local.at[4])
    spill.start()

    for s in range(1, narrow_n):
        for j in range(count):
            swap(s, j, lax.rem(me + narrow_n - s, narrow_n)).wait_recv()
    for copy in started[3:]:
        copy.wait()
    for q in range(PIECES):
        for j in range(fold):
            load_up(q, j).wait()

    def pair_copy(k):
        return pltpu.make_async_remote_copy(
            src_ref=csend.at[k],
            dst_ref=crecv.at[k],
            send_sem=rs_send.at[0, k],
            recv_sem=rs_recv.at[0, k],
            device_id={"wide": place(o, m, 1 - c)},
            device_id_type=MESH,
        )

    def side_copy(k):
        return pltpu.make_async_remote_copy(
            src_ref=xsend.at[k],
            dst_ref=xrecv.at[k],
            send_sem=rs_send.at[1, k],
            recv_sem=rs_recv.at[1, k],
            device_id={"wide": place(o, 1 - m, c)},
            device_id_type=MESH,
        )

    def long_copy(k):
        g = group_at(o, outer - 1 - k, outer)
        return pltpu.make_async_remote_copy(
            src_ref=zsend.at[k],
            dst_ref=zrecv.at[o],
            send_sem=rs_send.at[2, k],
            recv_sem=z_recv.at[o],
            device_id={"wide": place(g, m, c)},
            device_id_type=MESH,
        )

    def come(index):
        return pltpu.make_async_remote_copy(
            src_ref=zsend.at[0],
            dst_ref=zrecv.at[index],
            send_sem=rs_send.at[2, 0],
            recv_sem=z_recv.at[index],
            device_id={"wide": place(lax.rem(o + 1, outer), m, c)},
            device_id_type=MESH,
        )

    def piece_rows(mm, cc):
        return pl.ds(pl.multiple_of((mm * 2 + cc) * rows, rows), rows)

    def halve(k):
        for mm in range(2):
            csend[k, mm] = acc[piece_rows(mm, 1 - c), :].astype(BF16)
            keep[k, mm] = acc[piece_rows(mm, c), :]
        pair_copy(k).start()

    def across(k):
        pair_copy(k).wait_recv()
        xsend[k] = (keep[k, 1 - m] + crecv[k, 1 - m].astype(F32)).astype(BF16)
        side_copy(k).start()

    def along(k):
        side_copy(k).wait_recv()
        total = keep[k, m] + crecv[k, m].astype(F32) + xrecv[k].astype(F32)
        zsend[k] = total.astype(BF16)
        long_copy(k).start()

    def chip(k, mm):
        return keep[k, mm] + crecv[k, mm].astype(F32)

    def near():
        k = outer - 2
        pair_copy(k).wait_recv()
        give_out[1] = chip(k, 1 - m).astype(BF16)
        near_out[...] = chip(k, m)

    tall = min(2048, hidden)

    def exchange(i, carry):
        k, q = i // PIECES, i % PIECES
        a = outer - 1 - k
        for s in range(1, narrow_n):
            deal(s, k, q, a).wait_recv()
        span = pl.ds(pl.multiple_of(q * width, width), width)
        act = part[a, q]
        for s in range(1, narrow_n):
            act = act + other[s - 1, k, q].astype(F32)
        value, slope = gelu_parts(pre_all[rows_of(a), span])
        activ[rows_of(a), span] = value.astype(BF16)
        mine = (act * slope).astype(BF16)
        pgrad[rows_of(a), span] = mine

        def clear():
            acc[...] = jnp.zeros_like(acc)

        pl.when(q == 0)(clear)

        for j in range(fold):

            def strip(t, inner):
                out = pl.ds(pl.multiple_of(j * hidden + t * tall, tall), tall)
                acc[:, out] += lax.dot_general(
                    pgrad[rows_of(a), span],
                    w[
                        pl.ds(pl.multiple_of(t * tall, tall), tall),
                        pl.ds(pl.multiple_of(j * hidden + q * width, width), width),
                    ],
                    (((1,), (1,)), ((), ())),
                    preferred_element_type=F32,
                )
                return inner

            lax.fori_loop(0, hidden // tall, strip, 0)

        pl.when(q == PIECES - 1)(lambda: halve(k))
        inner = jnp.logical_and(k >= 1, k <= outer - 2)
        pl.when(jnp.logical_and(inner, q == 0))(lambda: across(k - 1))
        pl.when(jnp.logical_and(inner, q == PIECES - 1))(lambda: along(k - 1))

        def on(index, *events):
            def run():
                for event in events:
                    event()

            pl.when(i == index)(run)

        on(0, functools.partial(feeds.cross, 0), functools.partial(feeds.hop, 2))
        for step in range(3, outer):
            on(3 * step - 3, functools.partial(feeds.hop, step))
        for x in range(1, outer):
            on(3 * x, functools.partial(feeds.cross, x))
        on((outer - 1) * PIECES, near)
        return carry

    lax.fori_loop(0, outer * PIECES, exchange, 0)

    tail = [
        pltpu.make_async_copy(activ, activ_out, local.at[5]),
        pltpu.make_async_copy(pgrad, pgrad_out, local.at[6]),
    ]
    for copy in tail:
        copy.start()
    final = outer - 1
    pair_copy(final).wait_recv()
    give_out[0] = chip(final, 1 - m).astype(BF16)
    keep_out[...] = chip(final, m)
    for s in range(1, outer):
        index = lax.rem(o + s, outer)

        def take(index=index):
            come(index).wait_recv()
            keep_out[...] += zrecv[index].astype(F32)

        pl.when(group_at(index, 1, outer) != o)(take)

    for a in range(outer):
        feeds.finish(a)
    grads.drain()
    feeds.drain()
    for s in range(1, narrow_n):
        for j in range(count):
            swap(s, j, me).wait_send()
    for k in range(outer):
        for q in range(PIECES):
            for s in range(1, narrow_n):
                deal(s, k, q, 0).wait_send()
        pair_copy(k).wait_send()
        if k < outer - 2:
            side_copy(k).wait_send()
            long_copy(k).wait_send()
    started[2].wait()
    spill.wait()
    for copy in tail:
        copy.wait()


def core(out_grad, inputs, preact, w_down, w_up, outer, narrow_n):
    rows, cols = out_grad.shape
    block = 4 * rows
    tokens = block * outer
    hidden = preact.shape[1]
    width = hidden // PIECES
    count = preact.shape[0] // block
    slots = 2 * (outer - 1) + 3 * outer
    vmem, anywhere = (pl.BlockSpec(memory_space=space) for space in (pltpu.VMEM, pl.ANY))
    dma = pltpu.SemaphoreType.DMA
    return pl.pallas_call(
        functools.partial(core_kernel, outer, narrow_n),
        out_shape=(
            jax.ShapeDtypeStruct((tokens, cols), BF16),
            jax.ShapeDtypeStruct((tokens, cols), BF16),
            jax.ShapeDtypeStruct((tokens, hidden), BF16),
            jax.ShapeDtypeStruct((tokens, hidden), BF16),
            jax.ShapeDtypeStruct((rows, cols), F32),
            jax.ShapeDtypeStruct((rows, cols), F32),
            jax.ShapeDtypeStruct((2, rows, cols), BF16),
        ),
        in_specs=[anywhere] * 5,
        out_specs=(anywhere, anywhere, anywhere, anywhere, vmem, vmem, vmem),
        scratch_shapes=[
            pltpu.VMEM((hidden, cols), BF16),
            pltpu.VMEM((tokens, cols), BF16),
            pltpu.VMEM((outer, PIECES, block, width), F32),
            pltpu.VMEM((outer, PIECES, block, width), BF16),
            pltpu.VMEM((narrow_n - 1, outer, PIECES, block, width), BF16),
            pltpu.VMEM((tokens, hidden), BF16),
            pltpu.VMEM((tokens, hidden), BF16),
            pltpu.VMEM((tokens, hidden), BF16),
            pltpu.VMEM((block, cols), F32),
            pltpu.VMEM((outer, 2, rows, cols), F32),
            pltpu.VMEM((outer, 2, rows, cols), BF16),
            pltpu.VMEM((outer, 2, rows, cols), BF16),
            pltpu.VMEM((outer, rows, cols), BF16),
            pltpu.VMEM((outer, rows, cols), BF16),
            pltpu.VMEM((outer, rows, cols), BF16),
            pltpu.VMEM((outer, rows, cols), BF16),
            dma((2, slots)),
            dma((2, slots)),
            dma((narrow_n, count)),
            dma((narrow_n, count)),
            dma((narrow_n - 1, outer, PIECES)),
            dma((narrow_n - 1, outer, PIECES)),
            dma((3, outer)),
            dma((2, outer)),
            dma((outer,)),
            dma((PIECES, cols // hidden)),
            dma((7 + count,)),
        ],
        compiler_params=pltpu.CompilerParams(
            collective_id=0, has_side_effects=True, vmem_limit_bytes=58 * 2**20
        ),
    )(out_grad, inputs, preact, w_down, w_up)


def outer_product_kernel(a_ref, b_ref, o_ref):
    o_ref[...] = lax.dot_general(
        a_ref[...], b_ref[...], (((0,), (0,)), ((), ())), preferred_element_type=F32
    ).astype(BF16)


def outer_product(a, b, tile):
    t, d = a.shape
    f = b.shape[1]
    tile = min(tile, d)
    return pl.pallas_call(
        outer_product_kernel,
        grid=(d // tile,),
        in_specs=[
            pl.BlockSpec((t, tile), lambda i: (0, i)),
            pl.BlockSpec((t, f), lambda i: (0, 0)),
        ],
        out_specs=pl.BlockSpec((tile, f), lambda i: (i, 0)),
        out_shape=jax.ShapeDtypeStruct((d, f), BF16),
        compiler_params=pltpu.CompilerParams(vmem_limit_bytes=60 * 2**20),
        cost_estimate=pl.CostEstimate(
            flops=2 * t * d * f,
            bytes_accessed=2 * (t * d + t * f + d * f),
            transcendentals=0,
        ),
    )(a, b)


def shards(inputs, out_grad, preact, w_up, w_down):
    wide_n = lax.axis_size("wide")
    narrow_n = lax.axis_size("narrow")
    outer = wide_n // 4
    grad_all, inputs_all, activ, pgrad, keep, near, give = core(
        out_grad, inputs, preact, w_down, w_up, outer, narrow_n
    )
    got = lax.ppermute(give, "wide", [(i, i ^ 2) for i in range(wide_n)])
    up_grad = outer_product(inputs_all, pgrad, 1024)
    activ, got, _ = lax.optimization_barrier((activ, got, up_grad[:8, :128]))
    chain = (near + got[1].astype(F32)).astype(BF16)
    line = {o: o - 1 if o else 1 for o in range(outer)}
    hops = []
    for part in ([o for o in line if o != 2], [2]):
        pairs = [(4 * o + j, 4 * line[o] + j) for o in part for j in range(4)]
        hops.append(lax.ppermute(chain, "wide", pairs))
    down_grad = outer_product(activ, grad_all, 512)
    in_grad = keep + got[0].astype(F32)
    for hop in hops:
        in_grad = in_grad + hop.astype(F32)
    return (in_grad.astype(BF16), up_grad, down_grad)


def solution(mesh):
    in_specs = (
        P("wide", "narrow"),
        P("wide", "narrow"),
        P("narrow", "wide"),
        P("narrow", "wide"),
        P("wide", "narrow"),
    )
    out_specs = (P("wide", "narrow"), P("narrow", "wide"), P("wide", "narrow"))
    return jax.shard_map(shards, mesh=mesh, in_specs=in_specs, out_specs=out_specs, check_vma=False)
```
